32 devices in a mesh: comp: 8 (over y, x, core), samp: 4 (over z).
Axes of the slice: x: 2, y: 2, z: 4, core: 2. Of those that a mesh axis runs over, the one named last changes fastest.
Arguments:
- start_points: float32 [512, 512], P('samp'), may hold values from -6 to 6
- centers: bfloat16 [65536, 512], P('comp'), may hold values from -1.25 to 1.25
- log_weights: float32 [65536], P('comp'), may hold values from -6 to 6
- noise_draws: bfloat16 [6, 512, 512], P(None, 'samp'), may hold values from -6 to 6
Outputs:
- final_points: float32 [512, 512], P('samp')
- log_mass: float32 [512], P('samp')
- occupancy: float32 [65536], P('comp')
The draws below stay inside these ranges and needn't reach their ends.
All inputs are finite; a program needn't handle non-finite values.
Results may differ from the reference program's by a relative error of at most 0.0065.
Values sent between devices are 32-bit elements; how exact they have to be, the bound alone decides.
A program may use at most 128 MiB of HBM per device.

```python
import jax
import jax.numpy as jnp
from jax import lax

D = 512
K = 65536
BLOCK = 2048
STEPS = 6
SAMPLES = 512


def mixture_draw(key):
    key_base, key_sign, key_size, key_offset, key_points = jax.random.split(jax.random.fold_in(key, 11), 5)
    center_vals = 0.25 * jax.random.truncated_normal(key_base, -5.0, 5.0, (K, D), jnp.float32)
    point_vals = jax.random.truncated_normal(key_points, -6.0, 6.0, (SAMPLES, D), jnp.float32)
    return (center_vals, point_vals)


def draw_centers(key, part):
    return mixture_draw(key)[0].astype(jnp.bfloat16)


def draw_start_points(key, part):
    return mixture_draw(key)[1].astype(jnp.float32)


def level_of(stream_key, shape, shards, least, high):
    gain = 1.0
    for position, blocks in shards:
        draws = jax.random.uniform(jax.random.fold_in(jax.random.fold_in(stream_key, 6), position), (blocks,), jnp.float32, least / len(shards), high / len(shards))
        gain = gain * jnp.repeat(jnp.exp(draws), shape[position] // blocks).reshape((-1,) + (1,) * (len(shape) - 1 - position))
    return gain


def scatter_about(key, dims, width, bound, cuts=(), dtype=jnp.bfloat16):
    array = jax.random.normal(key, dims, jnp.float32) * width
    if len(cuts) > 0:
        array = level_of(key, dims, cuts, -0.22, 0.18) * array
    return jnp.clip(array, min=-bound, max=bound).astype(dtype)


def setup_inputs(seed: int = 0) -> dict:
    key_list = jax.random.split(jax.random.key(seed), 5)
    return {
        "start_points": draw_start_points(jax.random.fold_in(key_list[4], 71), 0),
        "centers": draw_centers(jax.random.fold_in(key_list[4], 71), 0),
        "log_weights": scatter_about(key_list[2], (K,), 1.0, 6.0, ((0, 8),), jnp.float32),
        "noise_draws": scatter_about(key_list[3], (STEPS, SAMPLES, D), 1.0, 6.0, ((1, 4),)),
    }


drift_rate = 0.5
noise_gain = 1.0


def block_scores(points_bf, center_block, bias_block):
    scores = lax.dot_general(points_bf, center_block, (((1,), (1,)), ((), ())), preferred_element_type=jnp.float32)
    return scores + bias_block[None, :]


def reference(start_points, centers, log_weights, noise_draws):
    center_f = centers.astype(jnp.float32)
    bias_all = log_weights - 0.5 * jnp.sum(center_f * center_f, axis=1)
    nblocks = K // BLOCK
    center_blocks = centers.reshape(nblocks, BLOCK, D)
    bias_blocks = bias_all.reshape(nblocks, BLOCK)
    points = start_points
    occupancy_sum = jnp.zeros((K,), jnp.float32)
    log_mass = jnp.zeros((start_points.shape[0],), jnp.float32)
    for step_index in range(STEPS):
        points_bf = points.astype(jnp.bfloat16)

        def partial_block(pair):
            center_block, bias_block = pair
            scores = block_scores(points_bf, center_block, bias_block)
            block_top = jnp.max(scores, axis=1)
            expd = jnp.exp(scores - block_top[:, None])
            block_mass = jnp.sum(expd, axis=1)
            pulled = jnp.dot(expd.astype(jnp.bfloat16), center_block, preferred_element_type=jnp.float32)
            return block_top, block_mass, pulled

        tops, masses, pulls = lax.map(partial_block, (center_blocks, bias_blocks))
        row_top = jnp.max(tops, axis=0)
        factors = jnp.exp(tops - row_top[None, :])
        total_mass = jnp.sum(factors * masses, axis=0)
        total_pull = jnp.sum(factors[:, :, None] * pulls, axis=0)
        log_mass = row_top + jnp.log(total_mass)

        def block_share(pair):
            center_block, bias_block = pair
            scores = block_scores(points_bf, center_block, bias_block)
            shares = jnp.exp(scores - row_top[:, None]) / total_mass[:, None]
            return jnp.sum(shares, axis=0)

        occupancy_sum = occupancy_sum + lax.map(block_share, (center_blocks, bias_blocks)).reshape(K)
        points = (1.0 - drift_rate) * points + drift_rate * (total_pull / total_mass[:, None]) + noise_gain * noise_draws[step_index].astype(jnp.float32)
    occupancy = occupancy_sum * (K / (SAMPLES * STEPS))
    return points, log_mass, occupancy
```

```python
import functools

import jax
import jax.numpy as jnp
from jax import lax
from jax.experimental import pallas as pl
from jax.experimental.pallas import tpu as pltpu
from jax.sharding import PartitionSpec as P

MESH = pl.DeviceIdType.MESH
LANES = 128
drift_rate = 0.5
noise_gain = 1.0


def lane_tiles(value):
    return [value[:, i : i + LANES] for i in range(0, value.shape[1], LANES)]


def kernel(
    n,
    zn,
    occ_scale,
    chunk,
    start_ref,
    centers_ref,
    lw_ref,
    noise_ref,
    points_out,
    logm_out,
    occ_out,
    cen,
    cent,
    bias,
    sco,
    pull,
    rbuf,
    stat_send,
    stat_buf,
    pts,
    occ,
    occ_buf,
    load_sem,
    rs_send,
    rs_recv,
    st_send,
    st_recv,
    ag_send,
    ag_recv,
    oc_send,
    oc_recv,
):
    rows, width = start_ref.shape
    kdev = centers_ref.shape[0]
    steps = noise_ref.shape[0]
    nchunks = kdev // chunk
    crows, cwidth = rbuf.shape[1], rbuf.shape[2]
    per_row = width // cwidth
    me = lax.axis_index("comp")
    mz = lax.axis_index("samp")

    def part(c):
        r = pl.multiple_of((c // per_row) * crows, crows)
        w = pl.multiple_of((c % per_row) * cwidth, cwidth)
        return pl.ds(r, crows), pl.ds(w, cwidth)

    def load(j):
        blk = pl.ds(j * chunk, chunk)
        return pltpu.make_async_copy(centers_ref.at[blk], cen.at[blk], load_sem.at[j])

    for j in range(nchunks):
        load(j).start()
    barrier = pltpu.get_barrier_semaphore()
    for k in range(1, n):
        pl.semaphore_signal(
            barrier, inc=1, device_id={"comp": lax.rem(me + k, n)}, device_id_type=MESH
        )
    for k in range(1, zn):
        pl.semaphore_signal(
            barrier, inc=1, device_id={"samp": lax.rem(mz + k, zn)}, device_id_type=MESH
        )
    pts[...] = start_ref[...]
    stat_send[...] = jnp.zeros_like(stat_send)
    occ[...] = jnp.zeros_like(occ)

    for j in range(nchunks):
        load(j).wait()
        blk = slice(j * chunk, (j + 1) * chunk)
        turned = cen[blk, :].T
        cent[:, blk] = turned
        wide = turned.astype(jnp.float32)
        bias[:, blk] = lw_ref[:, blk] - 0.5 * jnp.sum(wide * wide, axis=0, keepdims=True)
    pl.semaphore_wait(barrier, n - 1 + zn - 1)

    row_id = lax.broadcasted_iota(jnp.int32, (rows, LANES), 0)
    lane_id = lax.broadcasted_iota(jnp.int32, (rows, LANES), 1)
    eye = row_id == lane_id
    my_rows, my_cols = part(me)
    chunk_row = (
        lax.broadcasted_iota(jnp.int32, (crows, LANES), 0) + (me // per_row) * crows
    )
    chunk_eye = chunk_row == lax.broadcasted_iota(jnp.int32, (crows, LANES), 1)

    def rs_copy(peer_send, peer_recv):
        return pltpu.make_async_remote_copy(
            src_ref=pull.at[part(peer_send)],
            dst_ref=rbuf.at[me if peer_recv is None else peer_recv],
            send_sem=rs_send.at[peer_send],
            recv_sem=rs_recv.at[me if peer_recv is None else peer_recv],
            device_id={"comp": peer_send},
            device_id_type=MESH,
        )

    def st_copy(peer_send, peer_recv):
        slot = me if peer_recv is None else peer_recv
        return pltpu.make_async_remote_copy(
            src_ref=stat_send,
            dst_ref=stat_buf.at[slot],
            send_sem=st_send.at[peer_send],
            recv_sem=st_recv.at[slot],
            device_id={"comp": peer_send},
            device_id_type=MESH,
        )

    def ag_copy(peer_send, peer_recv):
        slot = me if peer_recv is None else peer_recv
        return pltpu.make_async_remote_copy(
            src_ref=pts.at[my_rows, my_cols],
            dst_ref=pts.at[part(slot)],
            send_sem=ag_send.at[peer_send],
            recv_sem=ag_recv.at[slot],
            device_id={"comp": peer_send},
            device_id_type=MESH,
        )

    def step(t, carry):
        points_bf = pts[...].astype(jnp.bfloat16)
        best = None
        for j in range(nchunks):
            blk = slice(j * chunk, (j + 1) * chunk)
            s = jnp.dot(points_bf, cent[:, blk], preferred_element_type=jnp.float32)
            s = s + bias[:, blk]
            sco[:, blk] = s
            local = functools.reduce(jnp.maximum, lane_tiles(s))
            best = local if best is None else jnp.maximum(best, local)
        top = jnp.max(best, axis=1, keepdims=True)
        mass = None
        acc = None
        for j in range(nchunks):
            blk = slice(j * chunk, (j + 1) * chunk)
            e = jnp.exp(sco[:, blk] - top)
            sco[:, blk] = e
            local = functools.reduce(jnp.add, lane_tiles(e))
            mass = local if mass is None else mass + local
            d = jnp.dot(
                e.astype(jnp.bfloat16), cen[blk, :], preferred_element_type=jnp.float32
            )
            acc = d if acc is None else acc + d
        pull[...] = acc
        total = jnp.sum(mass, axis=1, keepdims=True)
        stat_send[0:1, :] = jnp.sum(jnp.where(eye, top, 0.0), axis=0, keepdims=True)
        stat_send[1:2, :] = jnp.sum(jnp.where(eye, total, 0.0), axis=0, keepdims=True)
        for k in range(1, n):
            st_copy(lax.rem(me + k, n), None).start()
        for k in range(1, n):
            rs_copy(lax.rem(me + k, n), None).start()
        stat_buf[me] = stat_send[...]
        for k in range(1, n):
            st_copy(lax.rem(me + k, n), lax.rem(me + n - k, n)).wait_recv()

        tops = [stat_buf[d, 0:1, :] for d in range(n)]
        row_top = functools.reduce(jnp.maximum, tops)
        total_mass = functools.reduce(
            jnp.add,
            [jnp.exp(tops[d] - row_top) * stat_buf[d, 1:2, :] for d in range(n)],
        )
        logm_out[...] = row_top + jnp.log(total_mass)

        def gain(d):
            return jnp.exp(stat_buf[d, 0:1, :] - row_top) / total_mass

        def chunk_gain(d):
            return jnp.sum(jnp.where(chunk_eye, gain(d), 0.0), axis=1, keepdims=True)

        mine = pull[my_rows, my_cols] * chunk_gain(me)
        share = jnp.sum(jnp.where(eye, gain(me), 0.0), axis=1, keepdims=True)
        gains = [chunk_gain(lax.rem(me + n - k, n)) for k in range(1, n)]
        for k in range(1, n):
            src = lax.rem(me + n - k, n)
            rs_copy(lax.rem(me + k, n), src).wait_recv()
            mine = mine + rbuf[src] * gains[k - 1]
        pts[my_rows, my_cols] = (
            (1.0 - drift_rate) * pts[my_rows, my_cols]
            + drift_rate * mine
            + noise_gain * noise_ref[t, my_rows, my_cols].astype(jnp.float32)
        )
        for k in range(1, n):
            ag_copy(lax.rem(me + k, n), None).start()
        for j in range(nchunks):
            blk = slice(j * chunk, (j + 1) * chunk)
            o = sco[:, blk] * share
            occ[:, blk] += jnp.sum(o.reshape(rows // 8, 8, chunk), axis=0)
        for k in range(1, n):
            to, src = lax.rem(me + k, n), lax.rem(me + n - k, n)
            ag_copy(to, src).wait_recv()
            st_copy(to, src).wait_send()
            rs_copy(to, src).wait_send()
            ag_copy(to, src).wait_send()
        return carry

    lax.fori_loop(0, steps, step, 0)

    occ_buf[mz] = jnp.sum(occ[...], axis=0, keepdims=True)

    def oc_copy(to, slot):
        return pltpu.make_async_remote_copy(
            src_ref=occ_buf.at[mz],
            dst_ref=occ_buf.at[slot],
            send_sem=oc_send.at[to],
            recv_sem=oc_recv.at[slot],
            device_id={"samp": to},
            device_id_type=MESH,
        )

    for k in range(1, zn):
        oc_copy(lax.rem(mz + k, zn), mz).start()
    points_out[...] = pts[...]
    for k in range(1, zn):
        oc_copy(lax.rem(mz + k, zn), lax.rem(mz + zn - k, zn)).wait()
    occ_out[...] = functools.reduce(jnp.add, [occ_buf[d] for d in range(zn)]) * occ_scale


def body(n, zn, start_points, centers, log_weights, noise_draws):
    rows, width = start_points.shape
    kdev = centers.shape[0]
    steps = noise_draws.shape[0]
    crows = max(8, rows // n)
    cwidth = rows * width // (n * crows)
    chunk = min(1024, kdev)
    nchunks = kdev // chunk
    occ_scale = (kdev * n) / (rows * zn * steps)
    f32 = jnp.float32
    vmem = pl.BlockSpec(memory_space=pltpu.VMEM)
    dma = pltpu.SemaphoreType.DMA
    points, logm, occ = pl.pallas_call(
        functools.partial(kernel, n, zn, occ_scale, chunk),
        out_shape=(
            jax.ShapeDtypeStruct((rows, width), f32),
            jax.ShapeDtypeStruct((1, rows), f32),
            jax.ShapeDtypeStruct((1, kdev), f32),
        ),
        in_specs=[vmem, pl.BlockSpec(memory_space=pl.ANY), vmem, vmem],
        out_specs=(vmem, vmem, vmem),
        scratch_shapes=[
            pltpu.VMEM((kdev, width), jnp.bfloat16),
            pltpu.VMEM((width, kdev), jnp.bfloat16),
            pltpu.VMEM((1, kdev), f32),
            pltpu.VMEM((rows, kdev), f32),
            pltpu.VMEM((rows, width), f32),
            pltpu.VMEM((n, crows, cwidth), f32),
            pltpu.VMEM((8, rows), f32),
            pltpu.VMEM((n, 8, rows), f32),
            pltpu.VMEM((rows, width), f32),
            pltpu.VMEM((8, kdev), f32),
            pltpu.VMEM((zn, 1, kdev), f32),
            dma((nchunks,)),
            dma((n,)),
            dma((n,)),
            dma((n,)),
            dma((n,)),
            dma((n,)),
            dma((n,)),
            dma((zn,)),
            dma((zn,)),
        ],
        compiler_params=pltpu.CompilerParams(
            collective_id=0, has_side_effects=True, vmem_limit_bytes=60 * 1024 * 1024
        ),
    )(start_points, centers, log_weights.reshape(1, kdev), noise_draws)
    return points, logm.reshape(rows), occ.reshape(kdev)


def solution(mesh):
    n, zn = mesh.shape["comp"], mesh.shape["samp"]
    return jax.shard_map(
        functools.partial(body, n, zn),
        mesh=mesh,
        in_specs=(P("samp", None), P("comp", None), P("comp"), P(None, "samp", None)),
        out_specs=(P("samp", None), P("samp"), P("comp")),
        check_vma=False,
    )
```
